32 devices in a mesh: samples: 2 (over x), px: 8 (over z, y), py: 2 (over core).
Axes of the slice: x: 2, y: 2, z: 4, core: 2. Of those that a mesh axis runs over, the one named last changes fastest.
Arguments:
- source: float32 [2, 512, 256, 256], P(None, 'samples', 'px', 'py'), parts along dimension 1, may hold values from -6 to 6
- speed: float32 [512, 256, 256], P('samples', 'px', 'py'), parts along dimension 0, may hold values from 0.5 to 3
Outputs:
- solution: float32 [2, 512, 256, 256], P(None, 'samples', 'px', 'py'), parts along dimension 1
The draws below stay inside these ranges and needn't reach their ends.
There are 2 independent parts, one for each index of `samples`. The reference program is written for one: setup_inputs(seed, part) draws one part's arguments, and reference() takes and returns one part's arrays. A program takes and returns all parts, laid end to end along the dimension named above; each array names one. Nothing has to cross between parts.
All inputs are finite; a program needn't handle non-finite values.
Results may differ from the reference program's by a relative error of at most 0.00024.
Values sent between devices are 32-bit elements; how exact they have to be, the bound alone decides.
A program may use at most 192 MiB of HBM per device.

```python
import math
import jax
import jax.numpy as jnp
from jax import lax

NX = 256
NY = 256
NZ = 256


def draw_source(key, part):
    normal_part = jnp.clip(jax.random.normal(key, (2, NX, NY, NZ), jnp.float32), -6.0, 6.0)
    return normal_part


def level_of(own_key, extent, shards, low, largest):
    loudness, own = 1.0, jax.random.fold_in(own_key, 6)
    for position, parts in shards:
        heights = jnp.exp(jax.random.uniform(jax.random.fold_in(own, position), (parts,), jnp.float32, low / len(shards), largest / len(shards)))
        loudness = loudness * jnp.repeat(heights, extent[position] // parts).reshape([-1 if axis == position else 1 for axis in range(len(extent))])
    return loudness


def setup_inputs(seed: int = 0, part: int = 0) -> dict:
    key_list = jax.random.split(jax.random.key(seed), 3)
    part_splits = jax.random.split(jax.random.fold_in(key_list[2], part), 3)
    return {
        "source": draw_source(jax.random.fold_in(jax.random.fold_in(key_list[2], part), 71), part),
        "speed": jnp.clip(jnp.exp(math.log(3.0) - 1.7917595 * jax.random.uniform(part_splits[1], (NX, NY, NZ), jnp.float32) ** level_of(part_splits[1], (NX, NY, NZ), ((1, 8), (2, 2)), -0.2, 0.2)), 0.5, 3.0),
    }


wave_square = 0.25
damping = 0.5
epsilon = 1e-06
highest = lax.Precision.HIGHEST

def sine_table(length):
    positions = jnp.arange(length, dtype=jnp.float32) + 1.0
    phases = jnp.pi * positions[:, None] * positions[None, :] / (length + 1.0)
    return jnp.sqrt(2.0 / (length + 1.0)) * jnp.sin(phases)

def eigen_line(length, offset, number):
    positions = jnp.arange(number, dtype=jnp.float32) + jnp.asarray(offset).astype(jnp.float32) + 1.0
    sine_half = jnp.sin(jnp.pi * positions / (2.0 * (length + 1.0)))
    return 4.0 * sine_half * sine_half

def divide(values, eigen_x, eigen_y, eigen_z):
    shifted = eigen_x[:, None, None] + eigen_y[None, :, None] + eigen_z[None, None, :] - wave_square
    damped = damping * wave_square
    modulus = shifted * shifted + damped * damped
    real_part = (values[0] * shifted + values[1] * damped) / modulus
    imag_part = (values[1] * shifted - values[0] * damped) / modulus
    return jnp.stack([real_part, imag_part])

def transform(values, matrix_x, matrix_y, matrix_z):
    values = jnp.einsum('ak,ckyz->cayz', matrix_x, values, precision=highest)
    values = jnp.einsum('ak,cxkz->cxaz', matrix_y, values, precision=highest)
    return jnp.einsum('ak,cxyk->cxya', matrix_z, values, precision=highest)

def precondition(vector):
    matrix_x = sine_table(NX)
    matrix_y = sine_table(NY)
    matrix_z = sine_table(NZ)
    spectral = transform(vector, matrix_x, matrix_y, matrix_z)
    scaled = divide(spectral, eigen_line(NX, 0, NX), eigen_line(NY, 0, NY), eigen_line(NZ, 0, NZ))
    return transform(scaled, matrix_x, matrix_y, matrix_z)

def operate(vector, wave_field):
    padded = jnp.pad(vector, ((0, 0), (1, 1), (1, 1), (1, 1)))
    neighbours = padded[:, 2:, 1:-1, 1:-1] + padded[:, :-2, 1:-1, 1:-1]
    neighbours = neighbours + padded[:, 1:-1, 2:, 1:-1] + padded[:, 1:-1, :-2, 1:-1]
    neighbours = neighbours + padded[:, 1:-1, 1:-1, 2:] + padded[:, 1:-1, 1:-1, :-2]
    return (6.0 - wave_field) * vector - neighbours

def inner_sums(left, right):
    real_sum = jnp.sum(left[0] * right[0] + left[1] * right[1])
    imag_sum = jnp.sum(left[0] * right[1] - left[1] * right[0])
    return (real_sum, imag_sum)

def scaled_by(factor, vector):
    real_part = factor[0] * vector[0] - factor[1] * vector[1]
    imag_part = factor[0] * vector[1] + factor[1] * vector[0]
    return jnp.stack([real_part, imag_part])

def reference(source, speed):
    wave_field = wave_square / (speed * speed)
    source_size = jnp.sqrt(jnp.sum(source * source) + epsilon)
    basis_one = source / source_size
    solved_one = precondition(basis_one)
    applied = operate(solved_one, wave_field)
    one_re, one_im = inner_sums(basis_one, applied)
    remainder = applied - scaled_by((one_re, one_im), basis_one)
    two_one = jnp.sqrt(jnp.sum(remainder * remainder) + epsilon)
    denominator = one_re * one_re + one_im * one_im + two_one * two_one
    weight = (source_size * one_re / denominator, -source_size * one_im / denominator)
    return scaled_by(weight, solved_one)
```

```python
import functools

import jax
import jax.numpy as jnp
from jax import lax
from jax.experimental import pallas as pl
from jax.experimental.pallas import tpu as pltpu
from jax.sharding import PartitionSpec as P

wave_square = 0.25
damped = 0.125
epsilon = 1e-06
rows = 8
lanes = 128


def sine_table(length):
    index = jnp.arange(length, dtype=jnp.int32) + 1
    turns = (index[:, None] * index[None, :]) % (2 * (length + 1))
    phases = jnp.pi * turns.astype(jnp.float32) / (length + 1.0)
    return jnp.sqrt(2.0 / (length + 1.0)) * jnp.sin(phases)


def eigen_line(length):
    positions = jnp.arange(length, dtype=jnp.float32) + 1.0
    sine_half = jnp.sin(jnp.pi * positions / (2.0 * (length + 1.0)))
    return 4.0 * sine_half * sine_half


def halves(values):
    high = values.astype(jnp.bfloat16)
    low = (values - high.astype(jnp.float32)).astype(jnp.bfloat16)
    return high, low


def table_halves(table):
    high = lax.reduce_precision(table, exponent_bits=8, mantissa_bits=7)
    return high.astype(jnp.bfloat16), (table - high).astype(jnp.bfloat16)


def dot_three(left, right):
    dot = functools.partial(jnp.dot, preferred_element_type=jnp.float32)
    return dot(left[0], right[0]) + (dot(left[0], right[1]) + dot(left[1], right[0]))


def times(a, b):
    return a[0] * b[0] - a[1] * b[1], a[0] * b[1] + a[1] * b[0]


def plus(a, b):
    return a[0] + b[0], a[1] + b[1]


def inverse(a):
    scale = 1.0 / (a[0] * a[0] + a[1] * a[1])
    return a[0] * scale, -a[1] * scale


def next_pivot(diagonal, pivot):
    return inverse((diagonal - pivot[0], damped - pivot[1]))


def forward_x(x_ref, high_ref, low_ref, out_ref):
    _, length, _, _ = x_ref.shape
    flat = x_ref.at[0].reshape(length * rows, lanes)
    table = (high_ref[...], low_ref[...])
    parts, part = out_ref.shape[0], out_ref.shape[3]
    for j in range(0, rows, 2):
        pair = [flat[pl.ds(j + k, length, stride=rows), :] for k in range(2)]
        result = dot_three(table, halves(jnp.concatenate(pair, axis=1)))
        for k in range(2):
            for h in range(parts):
                out_ref[h, 0, j + k] = result[h * part : (h + 1) * part, k * lanes : (k + 1) * lanes]


def forward_z(t_ref, high_ref, low_ref, diagonal_ref, y_ref, ends_ref):
    parts, _, number, tile, _ = t_ref.shape
    modes = y_ref.shape[3]
    table = (high_ref[...], low_ref[...])
    for c in range(2):
        pieces = [t_ref[h, c].reshape(number * tile, lanes) for h in range(parts)]
        result = dot_three(halves(jnp.concatenate(pieces, axis=1)), table)
        y_ref[c] = result.reshape(number, tile, modes)
    diagonal = diagonal_ref[...]
    zero = jnp.zeros_like(diagonal)

    def step(j, state):
        pivot, product, last, first = state
        pivot = next_pivot(diagonal, pivot)
        last = times(plus((y_ref[0, j], y_ref[1, j]), last), pivot)
        first = plus(first, times(product, last))
        product = times(product, pivot)
        y_ref[0, j] = last[0]
        y_ref[1, j] = last[1]
        return pivot, product, last, first

    start = ((zero, zero), (zero + 1.0, zero), (zero, zero), (zero, zero))
    _, _, last, first = lax.fori_loop(0, number, step, start, unroll=2)
    for c in range(2):
        ends_ref[0, 0, c] = first[c]
        ends_ref[0, 1, c] = last[c]


def join(number, diagonal_ref, ends_ref, out_ref):
    count = ends_ref.shape[0]
    diagonal = diagonal_ref[...]
    zero = jnp.zeros_like(diagonal)

    def step(j, state):
        pivot = next_pivot(diagonal, state[0])
        return pivot, times(state[1], pivot)

    near, far = lax.fori_loop(0, number, step, ((zero, zero), (zero + 1.0, zero)))
    end, slope = (zero, zero), (zero, zero)
    saved = []
    for p in range(count):
        first = (ends_ref[p, 0, 0], ends_ref[p, 0, 1])
        last = (ends_ref[p, 1, 0], ends_ref[p, 1, 1])
        coupled = times(near, slope)
        quotient = inverse((1.0 - coupled[0], -coupled[1]))
        base = times(quotient, plus(first, times(near, end)))
        rate = times(quotient, far)
        saved.append((base, rate, end, slope))
        end, slope = (
            plus(last, times(far, plus(end, times(slope, base)))),
            plus(near, times(far, times(slope, rate))),
        )
    after = (zero, zero)
    for p in range(count - 1, -1, -1):
        base, rate, end, slope = saved[p]
        own = plus(base, times(rate, after))
        before = plus(end, times(slope, own))
        for c in range(2):
            out_ref[p, 0, c] = before[c]
            out_ref[p, 1, c] = after[c]
        after = own


def backward_z(y_ref, ends_ref, high_ref, low_ref, diagonal_ref, out_ref, pivots, products):
    parts, _, number, tile, _ = out_ref.shape
    modes = y_ref.shape[3]
    diagonal = diagonal_ref[...]
    zero = jnp.zeros_like(diagonal)
    before = (ends_ref[0, 0, 0], ends_ref[0, 0, 1])
    after = (ends_ref[0, 1, 0], ends_ref[0, 1, 1])

    def forward(j, state):
        pivot, carried = state
        pivot = next_pivot(diagonal, pivot)
        carried = times(carried, pivot)
        pivots[0, j] = pivot[0]
        pivots[1, j] = pivot[1]
        products[0, j] = y_ref[0, j] + carried[0]
        products[1, j] = y_ref[1, j] + carried[1]
        return pivot, carried

    lax.fori_loop(0, number, forward, ((zero, zero), before), unroll=2)

    def backward(i, value):
        j = number - 1 - i
        own = (products[0, j], products[1, j])
        value = plus(own, times((pivots[0, j], pivots[1, j]), value))
        products[0, j] = value[0]
        products[1, j] = value[1]
        return value

    lax.fori_loop(0, number, backward, after, unroll=2)
    table = (high_ref[...], low_ref[...])
    for c in range(2):
        result = dot_three(halves(products[c].reshape(number * tile, modes)), table)
        for h in range(parts):
            out_ref[h, c] = result[:, h * lanes : (h + 1) * lanes].reshape(number, tile, lanes)


def backward_x(t_ref, high_ref, low_ref, source_ref, speed_ref, w_ref, sums_ref):
    parts, _, _, _, _ = t_ref.shape
    length = speed_ref.shape[0]
    table = (high_ref[...], low_ref[...])
    flat = w_ref.reshape(2 * length * rows, lanes)
    for c in range(2):
        for j in range(0, rows, 2):
            pair = [
                jnp.concatenate([t_ref[h, c, j + k] for h in range(parts)], axis=0) for k in range(2)
            ]
            result = dot_three(table, halves(jnp.concatenate(pair, axis=1)))
            for k in range(2):
                flat[pl.ds(c * length * rows + j + k, length, stride=rows), :] = result[
                    :, k * lanes : (k + 1) * lanes
                ]

    @pl.when(pl.program_id(0) == 0)
    def _():
        sums_ref[...] = jnp.zeros_like(sums_ref)

    group = 8
    zero = jnp.zeros((rows, lanes), jnp.float32)

    def step(i, sums):
        part = pl.ds(i * group, group)
        speed = speed_ref[part]
        shift = wave_square - wave_square / (speed * speed)
        s_re, s_im, w_re, w_im = source_ref[0, part], source_ref[1, part], w_ref[0, part], w_ref[1, part]
        u_re = s_re + shift * w_re + damped * w_im
        u_im = s_im + shift * w_im - damped * w_re
        terms = (
            s_re * s_re + s_im * s_im,
            s_re * u_re + s_im * u_im,
            s_re * u_im - s_im * u_re,
            u_re * u_re + u_im * u_im,
        )
        return tuple(a + jnp.sum(b, axis=0) for a, b in zip(sums, terms))

    sums = lax.fori_loop(0, length // group, step, (zero,) * 4)
    for k in range(4):
        sums_ref[k] += sums[k]


def scale(weight_ref, w_ref, out_ref):
    re, im = weight_ref[0], weight_ref[1]
    out_ref[0] = re * w_ref[0] - im * w_ref[1]
    out_ref[1] = re * w_ref[1] + im * w_ref[0]


def on_device(blocks, parts, source, speed):
    _, length_x, number, width = source.shape
    length_z = width * parts
    part = length_x // parts
    tile = part // blocks
    steps = number // rows
    f32 = jnp.float32
    shape = jax.ShapeDtypeStruct
    whole = pl.BlockSpec((length_x, length_x), lambda *_: (0, 0))
    whole_z = pl.BlockSpec((length_z, length_z), lambda *_: (0, 0))
    sequential = lambda n: pltpu.CompilerParams(
        dimension_semantics=("arbitrary",) * n, vmem_limit_bytes=60000 * 1024
    )
    x_high, x_low = table_halves(sine_table(length_x))
    z_high, z_low = table_halves(sine_table(length_z))
    own = lax.dynamic_slice(eigen_line(length_x), (lax.axis_index("py") * part,), (part,))
    diagonal = (2.0 - wave_square) + own[:, None] + eigen_line(length_z)[None, :]

    sent = pl.pallas_call(
        forward_x,
        grid=(2, steps),
        in_specs=[pl.BlockSpec((1, length_x, rows, width), lambda c, y: (c, 0, y, 0)), whole, whole],
        out_specs=pl.BlockSpec((parts, 1, rows, part, width), lambda c, y: (0, c, y, 0, 0)),
        out_shape=shape((parts, 2, number, part, width), f32),
        compiler_params=sequential(2),
        name="forward_x",
    )(source, x_high, x_low)
    held = lax.all_to_all(sent, "py", split_axis=0, concat_axis=0, tiled=True)
    tiles = pl.BlockSpec((parts, 2, number, tile, width), lambda i: (0, 0, 0, i, 0))
    modes = pl.BlockSpec((2, number, tile, length_z), lambda i: (0, 0, i, 0))
    ends_spec = pl.BlockSpec((1, 2, 2, tile, length_z), lambda i: (i, 0, 0, 0, 0))
    line = pl.BlockSpec((tile, length_z), lambda i: (i, 0))
    swept, ends = pl.pallas_call(
        forward_z,
        grid=(blocks,),
        in_specs=[tiles, whole_z, whole_z, line],
        out_specs=[modes, ends_spec],
        out_shape=[
            shape((2, number, part, length_z), f32),
            shape((blocks, 2, 2, tile, length_z), f32),
        ],
        compiler_params=sequential(1),
        name="forward_z",
    )(held, z_high, z_low, diagonal)
    ends = lax.all_to_all(ends, "px", split_axis=0, concat_axis=0, tiled=True)
    mine = lax.dynamic_slice(diagonal, (lax.axis_index("px") * tile, 0), (tile, length_z))
    joined = pl.pallas_call(
        functools.partial(join, number),
        out_shape=shape(ends.shape, f32),
        name="join",
    )(mine, ends)
    joined = lax.all_to_all(joined, "px", split_axis=0, concat_axis=0, tiled=True)
    back = pl.pallas_call(
        backward_z,
        grid=(blocks,),
        in_specs=[modes, ends_spec, whole_z, whole_z, line],
        out_specs=tiles,
        out_shape=shape((parts, 2, number, part, width), f32),
        scratch_shapes=[pltpu.VMEM((2, number, tile, length_z), f32)] * 2,
        compiler_params=sequential(1),
        name="backward_z",
    )(swept, joined, z_high, z_low, diagonal)
    back = lax.all_to_all(back, "py", split_axis=0, concat_axis=0, tiled=True)
    block = pl.BlockSpec((2, length_x, rows, width), lambda y: (0, 0, y, 0))
    image, sums = pl.pallas_call(
        backward_x,
        grid=(steps,),
        in_specs=[
            pl.BlockSpec((parts, 2, rows, part, width), lambda y: (0, 0, y, 0, 0)),
            whole,
            whole,
            block,
            pl.BlockSpec((length_x, rows, width), lambda y: (0, y, 0)),
        ],
        out_specs=[block, pl.BlockSpec((4, rows, width), lambda y: (0, 0, 0))],
        out_shape=[shape(source.shape, f32), shape((4, rows, width), f32)],
        compiler_params=sequential(1),
        name="backward_x",
    )(back, x_high, x_low, source, speed)
    sums = lax.all_gather(jnp.sum(sums, axis=(1, 2)), ("px", "py"))
    sums = jnp.sum(sums, axis=0)
    size = sums[0] + epsilon
    one_re, one_im, squares = sums[1] / size, sums[2] / size, sums[3] / size
    one = one_re * one_re + one_im * one_im
    denominator = squares - one * (epsilon / size) + epsilon
    weight = jnp.stack([one_re / denominator, -one_im / denominator])
    cut = pl.BlockSpec((2, length_x // 8, number, width), lambda i: (0, i, 0, 0))
    return pl.pallas_call(
        scale,
        grid=(8,),
        in_specs=[pl.BlockSpec(memory_space=pltpu.SMEM), cut],
        out_specs=cut,
        out_shape=shape(source.shape, f32),
        compiler_params=sequential(1),
        name="scale",
    )(weight, image)


def solution(mesh):
    return jax.shard_map(
        functools.partial(on_device, mesh.shape["px"], mesh.shape["py"]),
        mesh=mesh,
        in_specs=(P(None, "samples", "px", "py"), P("samples", "px", "py")),
        out_specs=P(None, "samples", "px", "py"),
        check_vma=False,
    )
```

```python
import functools

import jax
import jax.numpy as jnp
from jax import lax
from jax.experimental import pallas as pl
from jax.experimental.pallas import tpu as pltpu
from jax.sharding import PartitionSpec as P

wave_square = 0.25
damped = 0.125
epsilon = 1e-06
rows = 8
lanes = 128
MESH = pl.DeviceIdType.MESH


def sine_table(length):
    index = jnp.arange(length, dtype=jnp.int32) + 1
    turns = (index[:, None] * index[None, :]) % (2 * (length + 1))
    phases = jnp.pi * turns.astype(jnp.float32) / (length + 1.0)
    return jnp.sqrt(2.0 / (length + 1.0)) * jnp.sin(phases)


def eigen_line(length):
    positions = jnp.arange(length, dtype=jnp.float32) + 1.0
    sine_half = jnp.sin(jnp.pi * positions / (2.0 * (length + 1.0)))
    return 4.0 * sine_half * sine_half


def halves(values):
    high = values.astype(jnp.bfloat16)
    low = (values - high.astype(jnp.float32)).astype(jnp.bfloat16)
    return high, low


def table_halves(table):
    high = lax.reduce_precision(table, exponent_bits=8, mantissa_bits=7)
    return high.astype(jnp.bfloat16), (table - high).astype(jnp.bfloat16)


def dot_three(left, right):
    dot = functools.partial(jnp.dot, preferred_element_type=jnp.float32)
    return dot(left[0], right[0]) + (dot(left[0], right[1]) + dot(left[1], right[0]))


def times(a, b):
    return a[0] * b[0] - a[1] * b[1], a[0] * b[1] + a[1] * b[0]


def plus(a, b):
    return a[0] + b[0], a[1] + b[1]


def inverse(a):
    scale = 1.0 / (a[0] * a[0] + a[1] * a[1])
    return a[0] * scale, -a[1] * scale


def next_pivot(diagonal, pivot):
    return inverse((diagonal - pivot[0], damped - pivot[1]))


def greet(peers):
    barrier = pltpu.get_barrier_semaphore()
    for peer in peers:
        pl.semaphore_signal(barrier, inc=1, device_id=peer, device_id_type=MESH)
    pl.semaphore_wait(barrier, len(peers))


def around(axis, size):
    me = lax.axis_index(axis)
    return me, [lax.rem(me + k, size) for k in range(1, size)]


def exchange(axis, peers, source, target, sends, receives):
    return [
        pltpu.make_async_remote_copy(
            src_ref=source(peer),
            dst_ref=target,
            send_sem=sends.at[k],
            recv_sem=receives.at[k],
            device_id={axis: peer},
            device_id_type=MESH,
        )
        for k, peer in enumerate(peers)
    ]


def hand_over(step, last, parts, slots, target_of, local_sem, sends, receives):
    me, peers = around("py", parts)

    def copies(i):
        mine = pltpu.make_async_copy(slots.at[i, me], target_of(me, i), local_sem.at[i])
        others = exchange(
            "py", peers, lambda peer: slots.at[i, peer], target_of(me, i), sends.at[i], receives.at[i]
        )
        return [mine] + others

    for copy in copies(step):
        copy.start()

    @pl.when(step == last)
    def _():
        @pl.loop(0, last + 1)
        def _(i):
            for copy in copies(i):
                copy.wait()


def forward_x(x_ref, high_ref, low_ref, out_ref, slots, local_sem, sends, receives):
    _, length, _, _ = x_ref.shape
    flat = x_ref.at[0].reshape(length * rows, lanes)
    table = (high_ref[...], low_ref[...])
    parts, part = out_ref.shape[0], out_ref.shape[3]
    steps = out_ref.shape[2] // rows
    now = pl.program_id(0) * steps + pl.program_id(1)

    @pl.when(now == 0)
    def _():
        greet([{"py": peer} for peer in around("py", parts)[1]])

    for j in range(0, rows, 2):
        pair = [flat[pl.ds(j + k, length, stride=rows), :] for k in range(2)]
        result = dot_three(table, halves(jnp.concatenate(pair, axis=1)))
        for k in range(2):
            for h in range(parts):
                slots[now, h, j + k] = result[h * part : (h + 1) * part, k * lanes : (k + 1) * lanes]

    def target_of(me, i):
        return out_ref.at[me, i // steps, pl.ds(lax.rem(i, steps) * rows, rows)]

    hand_over(now, 2 * steps - 1, parts, slots, target_of, local_sem, sends, receives)


def forward_z(t_ref, high_ref, low_ref, diagonal_ref, y_ref, ends_ref):
    parts, _, number, tile, _ = t_ref.shape
    modes = y_ref.shape[3]
    table = (high_ref[...], low_ref[...])
    for c in range(2):
        pieces = [t_ref[h, c].reshape(number * tile, lanes) for h in range(parts)]
        result = dot_three(halves(jnp.concatenate(pieces, axis=1)), table)
        y_ref[c] = result.reshape(number, tile, modes)
    diagonal = diagonal_ref[...]
    zero = jnp.zeros_like(diagonal)

    def step(j, state):
        pivot, product, last, first = state
        pivot = next_pivot(diagonal, pivot)
        last = times(plus((y_ref[0, j], y_ref[1, j]), last), pivot)
        first = plus(first, times(product, last))
        product = times(product, pivot)
        y_ref[0, j] = last[0]
        y_ref[1, j] = last[1]
        return pivot, product, last, first

    start = ((zero, zero), (zero + 1.0, zero), (zero, zero), (zero, zero))
    _, _, last, first = lax.fori_loop(0, number, step, start, unroll=2)
    for c in range(2):
        ends_ref[0, 0, c] = first[c]
        ends_ref[0, 1, c] = last[c]


def join(number, diagonal_ref, sent_ref, joined_ref, ends_ref, out_ref, local_sem, sends, receives):
    count = sent_ref.shape[0]
    me, peers = around("px", count)
    greet([{"px": peer} for peer in peers])
    copies = [pltpu.make_async_copy(sent_ref.at[me], ends_ref.at[me], local_sem.at[0])]
    copies += exchange(
        "px", peers, lambda peer: sent_ref.at[peer], ends_ref.at[me], sends.at[0], receives.at[0]
    )
    for copy in copies:
        copy.start()
    diagonal = diagonal_ref[...]
    zero = jnp.zeros_like(diagonal)

    def step(j, state):
        pivot = next_pivot(diagonal, state[0])
        return pivot, times(state[1], pivot)

    near, far = lax.fori_loop(0, number, step, ((zero, zero), (zero + 1.0, zero)))
    for copy in copies:
        copy.wait()
    end, slope = (zero, zero), (zero, zero)
    saved = []
    for p in range(count):
        first = (ends_ref[p, 0, 0], ends_ref[p, 0, 1])
        last = (ends_ref[p, 1, 0], ends_ref[p, 1, 1])
        coupled = times(near, slope)
        quotient = inverse((1.0 - coupled[0], -coupled[1]))
        base = times(quotient, plus(first, times(near, end)))
        rate = times(quotient, far)
        saved.append((base, rate, end, slope))
        end, slope = (
            plus(last, times(far, plus(end, times(slope, base)))),
            plus(near, times(far, times(slope, rate))),
        )
    after = (zero, zero)
    for p in range(count - 1, -1, -1):
        base, rate, end, slope = saved[p]
        own = plus(base, times(rate, after))
        before = plus(end, times(slope, own))
        for c in range(2):
            out_ref[p, 0, c] = before[c]
            out_ref[p, 1, c] = after[c]
        after = own
    copies = [pltpu.make_async_copy(out_ref.at[me], joined_ref.at[me], local_sem.at[1])]
    copies += exchange(
        "px", peers, lambda peer: out_ref.at[peer], joined_ref.at[me], sends.at[1], receives.at[1]
    )
    for copy in copies:
        copy.start()
    for copy in copies:
        copy.wait()


def backward_z(y_ref, ends_ref, high_ref, low_ref, diagonal_ref, out_ref, pivots, products, slots, local_sem, sends, receives):
    parts = out_ref.shape[0]
    _, number, tile, modes = y_ref.shape
    now, steps = pl.program_id(0), out_ref.shape[3] // tile

    @pl.when(now == 0)
    def _():
        greet([{"py": peer} for peer in around("py", parts)[1]])

    diagonal = diagonal_ref[...]
    zero = jnp.zeros_like(diagonal)
    before = (ends_ref[0, 0, 0], ends_ref[0, 0, 1])
    after = (ends_ref[0, 1, 0], ends_ref[0, 1, 1])

    def forward(j, state):
        pivot, carried = state
        pivot = next_pivot(diagonal, pivot)
        carried = times(carried, pivot)
        pivots[0, j] = pivot[0]
        pivots[1, j] = pivot[1]
        products[0, j] = y_ref[0, j] + carried[0]
        products[1, j] = y_ref[1, j] + carried[1]
        return pivot, carried

    lax.fori_loop(0, number, forward, ((zero, zero), before), unroll=2)

    def backward(i, value):
        j = number - 1 - i
        own = (products[0, j], products[1, j])
        value = plus(own, times((pivots[0, j], pivots[1, j]), value))
        products[0, j] = value[0]
        products[1, j] = value[1]
        return value

    lax.fori_loop(0, number, backward, after, unroll=2)
    table = (high_ref[...], low_ref[...])
    for c in range(2):
        result = dot_three(halves(products[c].reshape(number * tile, modes)), table)
        for h in range(parts):
            slots[now, h, c] = result[:, h * lanes : (h + 1) * lanes].reshape(number, tile, lanes)

    def target_of(me, i):
        return out_ref.at[me, :, :, pl.ds(pl.multiple_of(i * tile, tile), tile)]

    hand_over(now, steps - 1, parts, slots, target_of, local_sem, sends, receives)


def backward_x(t_ref, high_ref, low_ref, source_ref, speed_ref, w_ref, out_ref, sums_ref):
    parts, _, _, _, _ = t_ref.shape
    length = speed_ref.shape[0]
    table = (high_ref[...], low_ref[...])
    flat = w_ref.reshape(2 * length * rows, lanes)
    for c in range(2):
        for j in range(0, rows, 2):
            pair = [
                jnp.concatenate([t_ref[h, c, j + k] for h in range(parts)], axis=0) for k in range(2)
            ]
            result = dot_three(table, halves(jnp.concatenate(pair, axis=1)))
            for k in range(2):
                flat[pl.ds(c * length * rows + j + k, length, stride=rows), :] = result[
                    :, k * lanes : (k + 1) * lanes
                ]

    @pl.when(pl.program_id(0) == 0)
    def _():
        sums_ref[...] = jnp.zeros_like(sums_ref)

    group = 8
    zero = jnp.zeros((rows, lanes), jnp.float32)

    def step(i, sums):
        part = pl.ds(i * group, group)
        speed = speed_ref[part]
        shift = wave_square - wave_square / (speed * speed)
        s_re, s_im, w_re, w_im = source_ref[0, part], source_ref[1, part], w_ref[0, part], w_ref[1, part]
        u_re = s_re + shift * w_re + damped * w_im
        u_im = s_im + shift * w_im - damped * w_re
        terms = (
            s_re * s_re + s_im * s_im,
            s_re * u_re + s_im * u_im,
            s_re * u_im - s_im * u_re,
            u_re * u_re + u_im * u_im,
        )
        return tuple(a + jnp.sum(b, axis=0) for a, b in zip(sums, terms))

    sums = lax.fori_loop(0, length // group, step, (zero,) * 4)
    for k in range(4):
        sums_ref[k] += sums[k]

    @pl.when(pl.program_id(0) == pl.num_programs(0) - 1)
    def _():
        out_ref[...] = jnp.zeros_like(out_ref)
        for k in range(4):
            out_ref[pl.ds(k, 1)] = jnp.sum(sums_ref[k], axis=0, keepdims=True)


def total(blocks, parts, sums_ref, out_ref, slots, sends, receives):
    me = lax.axis_index("px") * parts + lax.axis_index("py")
    peers = []
    for k in range(1, blocks * parts):
        peer = lax.rem(me + k, blocks * parts)
        peers.append({"px": peer // parts, "py": lax.rem(peer, parts)})
    greet(peers)
    copies = [
        pltpu.make_async_remote_copy(
            src_ref=sums_ref,
            dst_ref=slots.at[k],
            send_sem=sends.at[k],
            recv_sem=receives.at[k],
            device_id=peer,
            device_id_type=MESH,
        )
        for k, peer in enumerate(peers)
    ]
    for copy in copies:
        copy.start()
    for copy in copies:
        copy.wait()
    out_ref[...] = sums_ref[...] + jnp.sum(slots[...], axis=0)


def scale(total_ref, w_ref, out_ref):
    sums = jnp.sum(total_ref[...], axis=1, keepdims=True)
    size = sums[0:1] + epsilon
    one_re, one_im, squares = sums[1:2] / size, sums[2:3] / size, sums[3:4] / size
    one = one_re * one_re + one_im * one_im
    denominator = squares - one * (epsilon / size) + epsilon
    spread = (w_ref.shape[2], lanes)
    re = jnp.broadcast_to(one_re / denominator, spread)
    im = jnp.broadcast_to(-one_im / denominator, spread)
    out_ref[0] = re * w_ref[0] - im * w_ref[1]
    out_ref[1] = re * w_ref[1] + im * w_ref[0]


def on_device(blocks, parts, source, speed):
    _, length_x, number, width = source.shape
    length_z = width * parts
    part = length_x // parts
    tile = part // blocks
    steps = number // rows
    f32 = jnp.float32
    shape = jax.ShapeDtypeStruct
    whole = pl.BlockSpec((length_x, length_x), lambda *_: (0, 0))
    whole_z = pl.BlockSpec((length_z, length_z), lambda *_: (0, 0))
    def sequential(n, number=None):
        remote = {} if number is None else {"collective_id": number, "has_side_effects": True}
        return pltpu.CompilerParams(
            dimension_semantics=("arbitrary",) * n, vmem_limit_bytes=60000 * 1024, **remote
        )

    def semaphores(steps):
        dma = pltpu.SemaphoreType.DMA
        return [dma((steps,)), dma((steps, parts - 1)), dma((steps, parts - 1))]

    anywhere = pl.BlockSpec(memory_space=pl.ANY)
    x_high, x_low = table_halves(sine_table(length_x))
    z_high, z_low = table_halves(sine_table(length_z))
    own = lax.dynamic_slice(eigen_line(length_x), (lax.axis_index("py") * part,), (part,))
    diagonal = (2.0 - wave_square) + own[:, None] + eigen_line(length_z)[None, :]

    held = pl.pallas_call(
        forward_x,
        grid=(2, steps),
        in_specs=[pl.BlockSpec((1, length_x, rows, width), lambda c, y: (c, 0, y, 0)), whole, whole],
        out_specs=anywhere,
        out_shape=shape((parts, 2, number, part, width), f32),
        scratch_shapes=[pltpu.VMEM((2 * steps, parts, rows, part, width), f32)] + semaphores(2 * steps),
        compiler_params=sequential(2, 0),
        name="forward_x",
    )(source, x_high, x_low)
    tiles = pl.BlockSpec((parts, 2, number, tile, width), lambda i: (0, 0, 0, i, 0))
    modes = pl.BlockSpec((2, number, tile, length_z), lambda i: (0, 0, i, 0))
    ends_spec = pl.BlockSpec((1, 2, 2, tile, length_z), lambda i: (i, 0, 0, 0, 0))
    line = pl.BlockSpec((tile, length_z), lambda i: (i, 0))
    swept, ends = pl.pallas_call(
        forward_z,
        grid=(blocks,),
        in_specs=[tiles, whole_z, whole_z, line],
        out_specs=[modes, ends_spec],
        out_shape=[
            shape((2, number, part, length_z), f32),
            shape((blocks, 2, 2, tile, length_z), f32),
        ],
        compiler_params=sequential(1),
        name="forward_z",
    )(held, z_high, z_low, diagonal)
    mine = lax.dynamic_slice(diagonal, (lax.axis_index("px") * tile, 0), (tile, length_z))
    joined = pl.pallas_call(
        functools.partial(join, number),
        in_specs=[pl.BlockSpec(memory_space=pltpu.VMEM)] * 2,
        out_specs=anywhere,
        out_shape=shape(ends.shape, f32),
        scratch_shapes=[pltpu.VMEM(ends.shape, f32)] * 2
        + [
            pltpu.SemaphoreType.DMA((2,)),
            pltpu.SemaphoreType.DMA((2, blocks - 1)),
            pltpu.SemaphoreType.DMA((2, blocks - 1)),
        ],
        compiler_params=sequential(0, 1),
        name="join",
    )(mine, ends)
    back = pl.pallas_call(
        backward_z,
        grid=(blocks,),
        in_specs=[modes, ends_spec, whole_z, whole_z, line],
        out_specs=anywhere,
        out_shape=shape((parts, 2, number, part, width), f32),
        scratch_shapes=[pltpu.VMEM((2, number, tile, length_z), f32)] * 2
        + [pltpu.VMEM((blocks, parts, 2, number, tile, width), f32)]
        + semaphores(blocks),
        compiler_params=sequential(1, 2),
        name="backward_z",
    )(swept, joined, z_high, z_low, diagonal)
    block = pl.BlockSpec((2, length_x, rows, width), lambda y: (0, 0, y, 0))
    image, sums = pl.pallas_call(
        backward_x,
        grid=(steps,),
        in_specs=[
            pl.BlockSpec((parts, 2, rows, part, width), lambda y: (0, 0, y, 0, 0)),
            whole,
            whole,
            block,
            pl.BlockSpec((length_x, rows, width), lambda y: (0, y, 0)),
        ],
        out_specs=[block, pl.BlockSpec((rows, width), lambda y: (0, 0))],
        out_shape=[shape(source.shape, f32), shape((rows, width), f32)],
        scratch_shapes=[pltpu.VMEM((4, rows, width), f32)],
        compiler_params=sequential(1),
        name="backward_x",
    )(back, x_high, x_low, source, speed)
    peers = blocks * parts - 1
    sums = pl.pallas_call(
        functools.partial(total, blocks, parts),
        in_specs=[pl.BlockSpec(memory_space=pltpu.VMEM)],
        out_specs=pl.BlockSpec(memory_space=pltpu.VMEM),
        out_shape=shape((rows, width), f32),
        scratch_shapes=[
            pltpu.VMEM((peers, rows, width), f32),
            pltpu.SemaphoreType.DMA((peers,)),
            pltpu.SemaphoreType.DMA((peers,)),
        ],
        compiler_params=sequential(0, 3),
        name="total",
    )(sums)
    cut = pl.BlockSpec((2, length_x // 8, number, width), lambda i: (0, i, 0, 0))
    return pl.pallas_call(
        scale,
        grid=(8,),
        in_specs=[pl.BlockSpec((rows, width), lambda i: (0, 0)), cut],
        out_specs=cut,
        out_shape=shape(source.shape, f32),
        compiler_params=sequential(1),
        name="scale",
    )(sums, image)


def solution(mesh):
    return jax.shard_map(
        functools.partial(on_device, mesh.shape["px"], mesh.shape["py"]),
        mesh=mesh,
        in_specs=(P(None, "samples", "px", "py"), P("samples", "px", "py")),
        out_specs=P(None, "samples", "px", "py"),
        check_vma=False,
    )
```
